32 devices in a mesh: wide: 2 (over x), narrow: 4 (over y, core), depth: 4 (over z).
Axes of the slice: x: 2, y: 2, z: 4, core: 2. Of those that a mesh axis runs over, the one named last changes fastest.
Arguments:
- hidden_in: bfloat16 [512, 4096], P(('wide', 'narrow'), 'depth'), may hold values from -36 to 36
- queries: bfloat16 [512, 4096], P('wide', ('narrow', 'depth')), may hold values from -8 to 8
- lang_ids: int32 [512], replicated, may hold values from 0 to 1
- owner_slot: int32 [2], replicated, may hold values from 0 to 1, each once
- enc_kv: bfloat16 [2, 2, 768, 4096], P('wide', None, None, ('narrow', 'depth')), may hold values from -7 to 7
- attn_proj: bfloat16 [4096, 4096], P(('narrow', 'depth')), may hold values from -0.09375 to 0.09375
- norm_gain: float32 [4096], replicated, may hold values from 0.25 to 1.75
- router_proj: float32 [4096, 4], replicated, may hold values from -0.09375 to 0.09375
- expert_ids: int32 [512, 2], P('wide'), may hold values from 0 to 3, all different within a row; in each aligned block of 64 rows (0 to 63, 64 to 127, ...) at most 48 rows name the same one
- proj_in: bfloat16 [4, 4096, 5120], P('narrow', None, 'depth'), may hold values from -0.09375 to 0.09375
- proj_out: bfloat16 [4, 5120, 4096], P('narrow', 'depth'), may hold values from -0.078125 to 0.078125
Outputs:
- layer_out: bfloat16 [512, 4096], P(('wide', 'narrow'), 'depth')
The draws below stay inside these ranges and needn't reach their ends.
Inputs may be any that keep to these rules, and one draw needn't show every extreme that they name: `owner_slot`: every slot once. `expert_ids`: each row names two different experts. Within each aligned block of 64 rows (the rows of one index of wide+narrow) no expert is named more than 48 times, a bound that some block reaches.
All inputs are finite; a program needn't handle non-finite values.
Results may differ from the reference program's by a relative error of at most 0.017.
Values may be sent and summed in bfloat16 or wider, within the bound.
A program may use at most 128 MiB of HBM per device.

```python
import math
import jax
import jax.numpy as jnp
import numpy as np
from jax import lax

D = 4096
HEADS = 64
HEAD_DIM = 64
FF = 5120
ENC = 768
TOK_DEV = 64
EXPERTS = 4
LANGS = 2
BATCH = 512
CAP = 48


def draw_queries(key, part):
    base_draw = 1.5 * jax.random.truncated_normal(jax.random.fold_in(key, 1), -4.0, 4.0, (BATCH, HEADS * HEAD_DIM), jnp.float32)
    return base_draw.astype(jnp.bfloat16)


def draw_enc_kv(key, part):
    width_all = HEADS * HEAD_DIM
    offset = jax.random.truncated_normal(jax.random.fold_in(key, 2), -3.0, 3.0, (LANGS, 1, width_all), jnp.float32)
    noise_part = jax.random.truncated_normal(jax.random.fold_in(key, 3), -4.0, 4.0, (LANGS, ENC, width_all), jnp.float32)
    value_part = offset + noise_part
    key_part = jax.random.truncated_normal(jax.random.fold_in(key, 4), -4.0, 4.0, (LANGS, ENC, width_all), jnp.float32)
    return jnp.stack([key_part, value_part], axis=1).astype(jnp.bfloat16)


def draw_hidden_in(key, part):
    base_draw = jax.random.truncated_normal(jax.random.fold_in(key, 5), -4.0, 4.0, (BATCH, D), jnp.float32)
    return base_draw.astype(jnp.bfloat16)


def plant(drawn, key, least, largest):
    longest = drawn.shape.index(max(drawn.shape))
    spots = []
    for shift in (0, 1):
        where = [jax.random.randint(jax.random.fold_in(key, axis), (), 0, length) for axis, length in enumerate(drawn.shape)]
        where[longest] = (where[longest] + shift) % drawn.shape[longest]
        spots.append(tuple(where))
    return drawn.at[spots[0]].set(least).at[spots[1]].set(largest)


def shard_levels(key, shape, shards, least, largest):
    def one(dim, shards_of):
        draws = jax.random.uniform(jax.random.fold_in(jax.random.fold_in(key, 6), dim), (shards_of,), jnp.float32, least / len(shards), largest / len(shards))
        return jnp.repeat(jnp.exp(draws), shape[dim] // shards_of).reshape((-1,) + (1,) * (len(shape) - dim - 1))

    level = one(*shards[0])
    for cut in shards[1:]:
        level = level * one(*cut)
    return level


def cumulative_ranks(amount, skew):
    loads = [(1 << 20) // math.isqrt(standing ** skew) + 1 for standing in range(1, amount + 1)]
    deviation = 1 + sum(loads) // (1 << 30)
    return np.cumsum(np.array([max(1, weight // deviation) for weight in loads]))


def ranked(stream_key, dims, count, slope):
    grid = cumulative_ranks(count, slope)
    ticket = jax.random.randint(jax.random.fold_in(stream_key, 1), dims, 0, int(grid[count - 1]))
    grade = jnp.searchsorted(jnp.asarray(grid, jnp.int32), ticket, side="right")
    return jax.random.permutation(jax.random.fold_in(stream_key, 2), count)[grade].astype(jnp.int32)


def shared_out(key, own, number, rows, number_of, top, limit, lean):
    order = jax.random.permutation(key, number_of)
    heavy_load, ordinary = portions_of(number_of, rows * top, limit, lean, True), portions_of(number_of, rows * top, limit, lean, False)
    places = jnp.arange(number_of)

    def named(tallies, rotation):
        used = int((tallies > 0).sum())
        fixed = max(1, used // 4)
        moved = fixed + (places - fixed + rotation * (used - fixed)) % max(1, number_of - fixed)
        return jnp.zeros((number_of,), jnp.int32).at[order[jnp.where(places < fixed, places, moved)]].set(jnp.asarray(tallies, jnp.int32))

    tallies = jnp.where(number % 4 == 0, named(heavy_load, number // 4), named(ordinary, number - number // 4 - 1))
    mixed = jax.random.permutation(jax.random.fold_in(own, 3), number_of)
    source_of, receiver = mixed[0:number_of // 2 * 2:2], mixed[1:number_of // 2 * 2:2]
    margin = jnp.minimum(tallies[source_of] - 1, limit - tallies[receiver]) // 2
    margin = jnp.where((source_of == order[0]) | (receiver == order[0]) | (tallies[receiver] == 0), 0, jnp.maximum(margin, 0))
    moved = jax.random.randint(jax.random.fold_in(own, 4), (number_of // 2,), 0, 1 << 20) % (margin + 1)
    tallies = tallies.at[source_of].add(-moved).at[receiver].add(moved)
    items = jnp.searchsorted(jnp.cumsum(tallies), jnp.arange(rows * top), side="right").astype(jnp.int32)
    table = items.reshape(top, rows).T
    table = table[jax.random.permutation(jax.random.fold_in(own, 1), rows)]
    rotation = jax.random.randint(jax.random.fold_in(own, 2), (rows, 1), 0, top)
    return jnp.take_along_axis(table, (jnp.arange(top)[None, :] + rotation) % top, axis=1)


def portions_of(amount, total, most, slope, full):
    loads = [(1 << 20) // math.isqrt(grade ** slope) + 1 for grade in range(1, amount + 1)]
    largest = most if full else min(most, max(-(-total // amount), total * loads[0] // sum(loads)))
    least = 1 if total - largest >= amount - 1 else 0
    holding, spare = [largest] + [least] * (amount - 1), total - largest - least * (amount - 1)
    while spare > 0:
        free = [i for i in range(1, amount) if holding[i] < largest] or [i for i in range(1, amount) if holding[i] < most]
        whole, remaining = sum([loads[i] for i in free]), spare
        for i in free:
            more = min(most - holding[i], max(1, remaining * loads[i] // whole), spare)
            holding[i] = holding[i] + more
            spare = spare - more
    return np.array(holding)


def normal_values(key, shape, spread, reach, split=(), held_as=jnp.bfloat16):
    entries = spread * jax.random.normal(key, shape, jnp.float32)
    if split:
        entries = entries * shard_levels(key, shape, split, -0.22, 0.18)
    return jnp.clip(entries, -reach, reach).astype(held_as)


def setup_inputs(seed: int = 0) -> dict:
    streams_of = jax.random.split(jax.random.key(seed), 12)
    hidden_in = draw_hidden_in(jax.random.fold_in(streams_of[11], 71), 0)
    queries = draw_queries(jax.random.fold_in(streams_of[11], 71), 0)
    lang_ids = plant(ranked(streams_of[2], (BATCH,), LANGS, 2), jax.random.fold_in(streams_of[2], 3), 0, LANGS - 1).astype(jnp.int32)
    owner_slot = jax.random.permutation(streams_of[3], LANGS).astype(jnp.int32)
    enc_kv = draw_enc_kv(jax.random.fold_in(streams_of[11], 71), 0)
    attn_proj = normal_values(streams_of[5], (HEADS * HEAD_DIM, D), (HEADS * HEAD_DIM) ** -0.5, 0.09375, ((0, 16),))
    norm_gain = jnp.clip(1.0 + 0.15 * jax.random.normal(streams_of[6], (D,), jnp.float32), 0.25, 1.75)
    router_proj = normal_values(streams_of[7], (D, EXPERTS), D ** -0.5, 0.09375, (), jnp.float32)
    expert_ids_keys = jax.random.split(jax.random.fold_in(streams_of[8], 1), BATCH // TOK_DEV)
    expert_ids_turns = jax.random.permutation(jax.random.fold_in(streams_of[8], 3), BATCH // TOK_DEV)
    expert_ids = jax.vmap(lambda own, number: shared_out(jax.random.fold_in(streams_of[8], 2), own, number, TOK_DEV, EXPERTS, 2, CAP, 2))(expert_ids_keys, expert_ids_turns).reshape((BATCH, 2))
    proj_in = normal_values(streams_of[9], (EXPERTS, D, FF), D ** -0.5, 0.09375, ((0, 4), (2, 4)))
    proj_out = normal_values(streams_of[10], (EXPERTS, FF, D), FF ** -0.5, 0.078125, ((0, 4), (1, 4)))
    return {"hidden_in": hidden_in, "queries": queries, "lang_ids": lang_ids, "owner_slot": owner_slot, "enc_kv": enc_kv, "attn_proj": attn_proj, "norm_gain": norm_gain, "router_proj": router_proj, "expert_ids": expert_ids, "proj_in": proj_in, "proj_out": proj_out}


norm_eps = 1e-06

def reference(hidden_in, queries, lang_ids, owner_slot, enc_kv, attn_proj, norm_gain, router_proj, expert_ids, proj_in, proj_out):
    holder = owner_slot[lang_ids].astype(jnp.int32)
    block_rows = math.gcd(BATCH, 512)

    def attend(element):
        query_part, slot_tags = element
        query_rows = query_part.astype(jnp.float32).reshape(block_rows, HEADS, HEAD_DIM)

        def per_slot(running_sum, position):
            kv_pair = lax.dynamic_index_in_dim(enc_kv, position, 0, keepdims=False).astype(jnp.float32)
            key_rows = kv_pair[0].reshape(ENC, HEADS, HEAD_DIM)
            value_rows = kv_pair[1].reshape(ENC, HEADS, HEAD_DIM)
            scores = jnp.einsum('rhd,khd->rhk', query_rows, key_rows) * HEAD_DIM ** (-0.5)
            weights = jnp.exp(scores - lax.optimization_barrier(jnp.max(scores, axis=2, keepdims=True)))
            denominator = lax.optimization_barrier(jnp.sum(weights, axis=2))
            rounded = lax.optimization_barrier(weights.astype(jnp.bfloat16)).astype(jnp.float32)
            context = jnp.einsum('rhk,khd->rhd', rounded, value_rows) / denominator[:, :, None]
            return (running_sum + jnp.where((slot_tags == position)[:, None, None], context, 0.0), None)
        start_sum = jnp.zeros((block_rows, HEADS, HEAD_DIM), jnp.float32)
        running_sum, _ = lax.scan(per_slot, start_sum, jnp.arange(LANGS, dtype=jnp.int32))
        return running_sum.reshape(block_rows, HEADS * HEAD_DIM)
    context = lax.map(attend, (queries.reshape(BATCH // block_rows, block_rows, HEADS * HEAD_DIM), holder.reshape(BATCH // block_rows, block_rows)))
    context = context.reshape(BATCH, HEADS * HEAD_DIM).astype(jnp.bfloat16)
    attn_out = jnp.dot(context, attn_proj, preferred_element_type=jnp.float32)
    residual = (hidden_in.astype(jnp.float32) + attn_out).astype(jnp.bfloat16)
    resid_f32 = residual.astype(jnp.float32)
    inv_norm = lax.rsqrt(lax.optimization_barrier(jnp.mean(resid_f32 * resid_f32, axis=1)) + norm_eps)
    normed = (resid_f32 * inv_norm[:, None] * norm_gain[None, :]).astype(jnp.bfloat16)
    logits = jnp.dot(normed.astype(jnp.float32), router_proj, precision=lax.Precision.HIGHEST)
    pick_mask = expert_ids[:, :, None] == jnp.arange(EXPERTS, dtype=jnp.int32)[None, None, :]
    own_logit = lax.optimization_barrier(jnp.sum(jnp.where(pick_mask, logits[:, None, :], 0.0), axis=2))
    gates = jax.nn.sigmoid(own_logit - own_logit[:, ::-1])
    expert_weight = lax.optimization_barrier(jnp.sum(jnp.where(pick_mask, gates[:, :, None], 0.0), axis=1))

    def add_expert(running_sum, position):
        first_proj = lax.dynamic_index_in_dim(proj_in, position, 0, keepdims=False)
        second_proj = lax.dynamic_index_in_dim(proj_out, position, 0, keepdims=False)
        hidden_act = jnp.dot(normed, first_proj, preferred_element_type=jnp.float32)
        hidden_act = jax.nn.gelu(hidden_act, approximate=True).astype(jnp.bfloat16)
        expert_out = jnp.dot(hidden_act, second_proj, preferred_element_type=jnp.float32)
        expert_share = lax.optimization_barrier(jnp.sum(jnp.where(jnp.arange(EXPERTS, dtype=jnp.int32)[None, :] == position, expert_weight, 0.0), axis=1))
        return (running_sum + expert_share[:, None] * expert_out, None)
    start_total = jnp.zeros((BATCH, D), jnp.float32)
    moe_out, _ = lax.scan(add_expert, start_total, jnp.arange(EXPERTS, dtype=jnp.int32))
    return (resid_f32 + moe_out).astype(jnp.bfloat16)
```

```python
import functools

import jax
import jax.numpy as jnp
from jax import lax
from jax.experimental import pallas as pl
from jax.experimental.pallas import tpu as pltpu
from jax.sharding import PartitionSpec as P

HEAD_DIM = 64
LANES = 128
CHUNKS = 4
norm_eps = 1e-06

F32 = jnp.float32
BF16 = jnp.bfloat16


def layer_kernel(
    sizes,
    holder_ref,
    q_ref,
    hid_ref,
    gain_ref,
    rout_ref,
    ids_ref,
    kv_hbm,
    ap_hbm,
    win_hbm,
    wout_hbm,
    out_ref,
    kv,
    ap,
    win,
    wout,
    qin,
    cret,
    cback,
    ctx,
    part,
    core_in,
    hi_in,
    dep_in,
    xg,
    nm,
    hact,
    load_sem,
    qs,
    qr,
    bs,
    br,
    core_s,
    core_r,
    hi_s,
    hi_r,
    dep_s,
    dep_r,
    agd_s,
    agd_r,
    agh_s,
    agh_r,
    agc_s,
    agc_r,
):
    W, H, D = sizes
    C = CHUNKS
    rows, feats = q_ref.shape
    tok, quarter = hid_ref.shape
    cw = quarter // C
    width = quarter * D
    experts = 2 * H
    w_at = lax.axis_index("wide")
    n_at = lax.axis_index("narrow")
    d_at = lax.axis_index("depth")
    hi = n_at // 2
    lo = n_at % 2

    def rem(v, m):
        return lax.rem(v, m)

    kv_load = pltpu.make_async_copy(kv_hbm.at[0], kv, load_sem.at[0])
    kv_load.start()
    ap_load = pltpu.make_async_copy(ap_hbm, ap, load_sem.at[1])
    ap_load.start()

    core_dev = {"narrow": hi * 2 + (1 - lo)}

    def hi_dev(s):
        return {"narrow": rem(hi + s, H) * 2 + lo}

    def dep_dev(s):
        return {"depth": rem(d_at + s, D)}

    def wide_dev(s):
        return {"wide": rem(w_at + s, W)}

    barrier = pltpu.get_barrier_semaphore()
    peers = [core_dev]
    peers += [hi_dev(s) for s in range(1, H)]
    peers += [dep_dev(s) for s in range(1, D)]
    peers += [wide_dev(s) for s in range(1, W)]
    for peer in peers:
        pl.semaphore_signal(barrier, inc=1, device_id=peer, device_id_type=pl.DeviceIdType.MESH)
    pl.semaphore_wait(barrier, len(peers))

    def remote(src, dst, ss, rs, dev):
        cp = pltpu.make_async_remote_copy(
            src_ref=src,
            dst_ref=dst,
            send_sem=ss,
            recv_sem=rs,
            device_id=dev,
            device_id_type=pl.DeviceIdType.MESH,
        )
        cp.start()
        return cp

    sent = []

    q_copies = [
        remote(q_ref, qin.at[s - 1], qs.at[s - 1], qr.at[s - 1], wide_dev(s)) for s in range(1, W)
    ]
    win_load = pltpu.make_async_copy(win_hbm.at[0], win, load_sem.at[2])
    win_load.start()
    wout_load = pltpu.make_async_copy(wout_hbm.at[0], wout, load_sem.at[3])
    wout_load.start()
    kv_load.wait()

    lane = lax.broadcasted_iota(jnp.int32, (rows, LANES), 1)
    per = LANES // HEAD_DIM

    def attend(src, dst):
        def group(g, carry):
            at = pl.ds(pl.multiple_of(g * LANES, LANES), LANES)
            keys = kv[0, :, at]
            vals = kv[1, :, at]
            qg = src[:, at].astype(F32)
            out = jnp.zeros((rows, LANES), F32)
            for h in range(per):
                mine = (lane >= h * HEAD_DIM) & (lane < (h + 1) * HEAD_DIM)
                qh = jnp.where(mine, qg, 0.0).astype(BF16)
                scores = lax.dot_general(
                    qh, keys, (((1,), (1,)), ((), ())), preferred_element_type=F32
                ) * HEAD_DIM ** (-0.5)
                top = jnp.max(scores, axis=1, keepdims=True)
                wts = jnp.exp(scores - top)
                den = jnp.sum(wts, axis=1, keepdims=True)
                got = jnp.dot(wts.astype(BF16), vals, preferred_element_type=F32)
                out = jnp.where(mine, got / den, out)
            dst[:, at] = out.astype(BF16)
            return carry

        lax.fori_loop(0, feats // LANES, group, 0)

    attend(q_ref, ctx)
    back = []
    for s in range(1, W):
        q_copies[s - 1].wait_recv()
        attend(qin.at[s - 1], cret.at[s - 1])
        back.append(
            remote(cret.at[s - 1], cback.at[s - 1], bs.at[s - 1], br.at[s - 1], wide_dev(W - s))
        )
    ap_load.wait()
    tag = holder_ref[...]
    for s in range(1, W):
        back[s - 1].wait_recv()
        other = rem(w_at + s, W)
        ctx[...] = jnp.where(
            tag == other, cback[s - 1].astype(F32), ctx[...].astype(F32)
        ).astype(BF16)
    sent += q_copies + back

    def scatter_sum(k, produce, consume):
        copies = []
        core_cp = []
        hi_cp = []
        for c in range(C + 1):
            if c < C:
                produce(c)
                core_cp.append(
                    remote(
                        part.at[c, 1 - lo], core_in.at[k, c], core_s.at[k, c], core_r.at[k, c], core_dev
                    )
                )
            if c > 0:
                b = c - 1
                core_cp[b].wait_recv()
                part[b, lo] = (part[b, lo].astype(F32) + core_in[k, b].astype(F32)).astype(BF16)
                hi_cp.append(
                    [
                        remote(
                            part.at[b, lo, rem(hi + s, H)],
                            hi_in.at[k, b, s - 1],
                            hi_s.at[k, b, s - 1],
                            hi_r.at[k, b, s - 1],
                            hi_dev(s),
                        )
                        for s in range(1, H)
                    ]
                )
        dep_cp = []
        for c in range(C):
            held = part[c, lo, hi].astype(F32)
            for s in range(1, H):
                hi_cp[c][s - 1].wait_recv()
                held = held + hi_in[k, c, s - 1].astype(F32)
            part[c, lo, hi] = held.astype(BF16)
            dep_cp.append(
                [
                    remote(
                        part.at[c, lo, hi, rem(d_at + s, D)],
                        dep_in.at[k, c, s - 1],
                        dep_s.at[k, c, s - 1],
                        dep_r.at[k, c, s - 1],
                        dep_dev(s),
                    )
                    for s in range(1, D)
                ]
            )
        for c in range(C):
            held = part[c, lo, hi, d_at].astype(F32)
            for s in range(1, D):
                dep_cp[c][s - 1].wait_recv()
                held = held + dep_in[k, c, s - 1].astype(F32)
            consume(c, held)
        for c in range(C):
            copies += [core_cp[c]] + hi_cp[c] + dep_cp[c]
        return copies

    def store_part(c, q, tile):
        for n in range(2 * H):
            part[c, n % 2, n // 2, q] = tile[n * tok : (n + 1) * tok].astype(BF16)

    def project(c):
        def one(q, carry):
            at = pl.ds(pl.multiple_of(q * quarter + c * cw, LANES), cw)
            store_part(c, q, jnp.dot(ctx[...], ap[:, at], preferred_element_type=F32))
            return carry

        lax.fori_loop(0, D, one, 0)

    dep_ag = {}
    hi_ag = {}
    core_ag = {}

    def forward_hi(j, c):
        q = rem(d_at + D - j, D)
        for s in range(1, H):
            hi_ag[s, j, c] = remote(
                xg.at[lo, hi, q, c],
                xg.at[lo, hi, q, c],
                agh_s.at[s - 1, j, c],
                agh_r.at[s - 1, j, c],
                hi_dev(s),
            )

    def forward_core(i, j, c):
        q = rem(d_at + D - j, D)
        h = rem(hi + H - i, H)
        core_ag[i, j, c] = remote(
            xg.at[lo, h, q, c],
            xg.at[lo, h, q, c],
            agc_s.at[i, j, c],
            agc_r.at[i, j, c],
            core_dev,
        )

    def add_residual(c, total):
        res = hid_ref[:, c * cw : (c + 1) * cw].astype(F32) + total
        xg[lo, hi, d_at, c] = res.astype(BF16)
        for s in range(1, D):
            dep_ag[s, c] = remote(
                xg.at[lo, hi, d_at, c],
                xg.at[lo, hi, d_at, c],
                agd_s.at[s - 1, c],
                agd_r.at[s - 1, c],
                dep_dev(s),
            )
        forward_hi(0, c)
        forward_core(0, 0, c)

    first = scatter_sum(0, project, add_residual)

    for j in range(1, D):
        for c in range(C):
            dep_ag[j, c].wait_recv()
            forward_hi(j, c)
            forward_core(0, j, c)
    for j in range(D):
        for c in range(C):
            for s in range(1, H):
                hi_ag[s, j, c].wait_recv()
                forward_core(s, j, c)
    for key in core_ag:
        core_ag[key].wait_recv()

    def norm_block(n, carry):
        l = n % 2
        h = n // 2
        acc = jnp.zeros((tok, cw), F32)
        for q in range(D):
            for c in range(C):
                x = xg[l, h, q, c].astype(F32)
                acc = acc + x * x
        inv = lax.rsqrt(jnp.sum(acc, axis=1, keepdims=True) * (1.0 / width) + norm_eps)
        at_rows = pl.ds(pl.multiple_of(n * tok, tok), tok)
        for q in range(D):
            for c in range(C):
                at = q * quarter + c * cw
                x = xg[l, h, q, c].astype(F32)
                nm[at_rows, at : at + cw] = (x * inv * gain_ref[:, at : at + cw]).astype(BF16)
        return carry

    lax.fori_loop(0, 2 * H, norm_block, 0)

    pieces = lax.dot_general(
        nm[...], rout_ref[...], (((1,), (1,)), ((), ())), preferred_element_type=F32
    )
    column = lax.broadcasted_iota(jnp.int32, pieces.shape, 1)
    named = rem(column, experts)
    ids = ids_ref[...]
    id0 = ids[:, 0:1]
    id1 = ids[:, 1:2]
    logit0 = jnp.sum(jnp.where(named == id0, pieces, 0.0), axis=1, keepdims=True)
    logit1 = jnp.sum(jnp.where(named == id1, pieces, 0.0), axis=1, keepdims=True)
    gate0 = 1.0 / (1.0 + jnp.exp(logit1 - logit0))
    gate1 = 1.0 / (1.0 + jnp.exp(logit0 - logit1))
    gate = jnp.where(id0 == n_at, gate0, 0.0) + jnp.where(id1 == n_at, gate1, 0.0)

    win_load.wait()
    hidden = win.shape[1]
    step = 256 if hidden % 256 == 0 else LANES

    def enter(i, carry):
        at = pl.ds(pl.multiple_of(i * step, LANES), step)
        v = jnp.dot(nm[...], win[:, at], preferred_element_type=F32)
        act = 0.5 * v * (1.0 + jnp.tanh((2.0 / jnp.pi) ** 0.5 * (v + 0.044715 * v * v * v)))
        hact[:, at] = act.astype(BF16)
        return carry

    lax.fori_loop(0, hidden // step, enter, 0)

    for cp in first:
        cp.wait_send()
    wout_load.wait()

    def leave(c):
        def one(q, carry):
            at = pl.ds(pl.multiple_of(q * quarter + c * cw, LANES), cw)
            tile = jnp.dot(hact[...], wout[:, at], preferred_element_type=F32)
            store_part(c, q, tile * gate)
            return carry

        lax.fori_loop(0, D, one, 0)

    def finish(c, total):
        out_ref[:, c * cw : (c + 1) * cw] = (xg[lo, hi, d_at, c].astype(F32) + total).astype(BF16)

    second = scatter_sum(1, leave, finish)

    sent += second
    sent += list(dep_ag.values()) + list(hi_ag.values()) + list(core_ag.values())
    for cp in sent:
        cp.wait_send()


def shards(
    hidden_in,
    queries,
    lang_ids,
    owner_slot,
    enc_kv,
    attn_proj,
    norm_gain,
    router_proj,
    expert_ids,
    proj_in,
    proj_out,
):
    W = lax.axis_size("wide")
    N = lax.axis_size("narrow")
    D = lax.axis_size("depth")
    H = N // 2
    C = CHUNKS
    rows, feats = queries.shape
    tok, quarter = hidden_in.shape
    cw = quarter // C
    width = quarter * D
    langs = owner_slot.shape[0]
    assert langs == W and enc_kv.shape[0] == 1 and proj_in.shape[0] == 1 and N % 2 == 0
    own_lang = lax.dynamic_slice_in_dim(lang_ids, lax.axis_index("wide") * rows, rows)
    match = own_lang[:, None] == jnp.arange(langs, dtype=jnp.int32)[None, :]
    holder = jnp.sum(jnp.where(match, owner_slot[None, :], 0), axis=1, keepdims=True)
    experts = router_proj.shape[1]
    by_expert = router_proj.T
    high = lax.reduce_precision(by_expert, 8, 7)
    left = by_expert - high
    middle = lax.reduce_precision(left, 8, 7)
    low = left - middle
    fill = -(3 * experts) % 16
    router = jnp.concatenate(
        [high, middle, low, jnp.zeros((fill, by_expert.shape[1]), F32)], axis=0
    ).astype(BF16)
    hidden = proj_in.shape[2]
    keys = enc_kv.shape[2]
    dma = pltpu.SemaphoreType.DMA
    vmem = pl.BlockSpec(memory_space=pltpu.VMEM)
    hbm = pl.BlockSpec(memory_space=pl.ANY)
    return pl.pallas_call(
        functools.partial(layer_kernel, (W, H, D)),
        out_shape=jax.ShapeDtypeStruct((tok, quarter), BF16),
        in_specs=[vmem] * 6 + [hbm] * 4,
        out_specs=vmem,
        scratch_shapes=[
            pltpu.VMEM((2, keys, feats), BF16),
            pltpu.VMEM(attn_proj.shape, BF16),
            pltpu.VMEM(proj_in.shape[1:], BF16),
            pltpu.VMEM(proj_out.shape[1:], BF16),
            pltpu.VMEM((W - 1, rows, feats), BF16),
            pltpu.VMEM((W - 1, rows, feats), BF16),
            pltpu.VMEM((W - 1, rows, feats), BF16),
            pltpu.VMEM((rows, feats), BF16),
            pltpu.VMEM((C, 2, H, D, tok, cw), BF16),
            pltpu.VMEM((2, C, H, D, tok, cw), BF16),
            pltpu.VMEM((2, C, H - 1, D, tok, cw), BF16),
            pltpu.VMEM((2, C, D - 1, tok, cw), BF16),
            pltpu.VMEM((2, H, D, C, tok, cw), BF16),
            pltpu.VMEM((rows, width), BF16),
            pltpu.VMEM((rows, hidden), BF16),
            dma((4,)),
            dma((W - 1,)),
            dma((W - 1,)),
            dma((W - 1,)),
            dma((W - 1,)),
            dma((2, C)),
            dma((2, C)),
            dma((2, C, H - 1)),
            dma((2, C, H - 1)),
            dma((2, C, D - 1)),
            dma((2, C, D - 1)),
            dma((D - 1, C)),
            dma((D - 1, C)),
            dma((H - 1, D, C)),
            dma((H - 1, D, C)),
            dma((H, D, C)),
            dma((H, D, C)),
        ],
        compiler_params=pltpu.CompilerParams(
            collective_id=0, has_side_effects=True, vmem_limit_bytes=67043328
        ),
    )(
        holder,
        queries,
        hidden_in,
        norm_gain.reshape(1, width),
        router,
        expert_ids,
        enc_kv,
        attn_proj,
        proj_in,
        proj_out,
    )


def solution(mesh):
    return jax.shard_map(
        shards,
        mesh=mesh,
        in_specs=(
            P(("wide", "narrow"), "depth"),
            P("wide", ("narrow", "depth")),
            P(),
            P(),
            P("wide", None, None, ("narrow", "depth")),
            P(("narrow", "depth"), None),
            P(),
            P(),
            P("wide", None),
            P("narrow", None, "depth"),
            P("narrow", "depth", None),
        ),
        out_specs=P(("wide", "narrow"), "depth"),
        check_vma=False,
    )
```

```python
import functools

import jax
import jax.numpy as jnp
from jax import lax
from jax.experimental import pallas as pl
from jax.experimental.pallas import tpu as pltpu
from jax.sharding import PartitionSpec as P

HEAD_DIM = 64
LANES = 128
CHUNKS = 4
norm_eps = 1e-06

F32 = jnp.float32
BF16 = jnp.bfloat16


def layer_kernel(
    sizes,
    owner_ref,
    lang_ref,
    q_ref,
    hid_ref,
    gain_ref,
    router_ref,
    ids_ref,
    kv_hbm,
    ap_hbm,
    win_hbm,
    wout_hbm,
    out_ref,
    kv,
    ap,
    win,
    wout,
    qin,
    cret,
    cback,
    ctx,
    part,
    core_in,
    hi_in,
    dep_in,
    xg,
    nm,
    hact,
    rout,
    early_in,
    late_in,
    ed_s,
    ed_r,
    eh_s,
    eh_r,
    load_sem,
    qs,
    qr,
    bs,
    br,
    core_s,
    core_r,
    hi_s,
    hi_r,
    dep_s,
    dep_r,
    agd_s,
    agd_r,
    agh_s,
    agh_r,
    agc_s,
    agc_r,
):
    W, H, D = sizes
    C = CHUNKS
    rows, feats = q_ref.shape
    tok, quarter = hid_ref.shape
    cw = quarter // C
    width = quarter * D
    experts = 2 * H
    w_at = lax.axis_index("wide")
    n_at = lax.axis_index("narrow")
    d_at = lax.axis_index("depth")
    hi = n_at // 2
    lo = n_at % 2

    def rem(v, m):
        return lax.rem(v, m)

    kv_load = pltpu.make_async_copy(kv_hbm.at[0], kv, load_sem.at[0])
    kv_load.start()
    ap_load = pltpu.make_async_copy(ap_hbm, ap, load_sem.at[1])
    ap_load.start()

    core_dev = {"narrow": hi * 2 + (1 - lo)}

    def hi_dev(s):
        return {"narrow": rem(hi + s, H) * 2 + lo}

    def dep_dev(s):
        return {"depth": rem(d_at + s, D)}

    def wide_dev(s):
        return {"wide": rem(w_at + s, W)}

    barrier = pltpu.get_barrier_semaphore()
    peers = [core_dev]
    peers += [hi_dev(s) for s in range(1, H)]
    peers += [dep_dev(s) for s in range(1, D)]
    peers += [wide_dev(s) for s in range(1, W)]
    for peer in peers:
        pl.semaphore_signal(barrier, inc=1, device_id=peer, device_id_type=pl.DeviceIdType.MESH)
    pl.semaphore_wait(barrier, len(peers))

    def remote(src, dst, ss, rs, dev):
        cp = pltpu.make_async_remote_copy(
            src_ref=src,
            dst_ref=dst,
            send_sem=ss,
            recv_sem=rs,
            device_id=dev,
            device_id_type=pl.DeviceIdType.MESH,
        )
        cp.start()
        return cp

    sent = []

    groups = feats // LANES

    def lanes_of(g):
        return pl.ds(g * LANES, LANES)

    q_copies = [
        remote(
            q_ref.at[:, lanes_of(g)],
            qin.at[s - 1, :, lanes_of(g)],
            qs.at[s - 1, g],
            qr.at[s - 1, g],
            wide_dev(s),
        )
        for s in range(1, W)
        for g in range(groups)
    ]
    win_load = pltpu.make_async_copy(win_hbm.at[0], win, load_sem.at[2])
    win_load.start()
    wout_load = pltpu.make_async_copy(wout_hbm.at[0], wout, load_sem.at[3])
    wout_load.start()
    kv_load.wait()

    diagonal = lax.broadcasted_iota(jnp.int32, (rows, rows), 0) == lax.broadcasted_iota(
        jnp.int32, (rows, rows), 1
    )

    def to_column(row):
        return jnp.sum(jnp.where(diagonal, row, 0), axis=1, keepdims=True)

    router = router_ref[...]
    high = router.astype(BF16).astype(F32)
    left = router - high
    middle = left.astype(BF16).astype(F32)
    rout[...] = jnp.zeros_like(rout)
    rout[0:experts] = high
    rout[experts : 2 * experts] = middle
    rout[2 * experts : 3 * experts] = left - middle

    lane = lax.broadcasted_iota(jnp.int32, (rows, LANES), 1)
    per = LANES // HEAD_DIM

    def attend(src, dst, first, last):
        def group(g, carry):
            at = pl.ds(pl.multiple_of(g * LANES, LANES), LANES)
            keys = kv[0, :, at]
            vals = kv[1, :, at]
            qg = src[:, at].astype(F32)
            out = jnp.zeros((rows, LANES), F32)
            for h in range(per):
                mine = (lane >= h * HEAD_DIM) & (lane < (h + 1) * HEAD_DIM)
                qh = jnp.where(mine, qg, 0.0).astype(BF16)
                scores = lax.dot_general(
                    qh, keys, (((1,), (1,)), ((), ())), preferred_element_type=F32
                ) * HEAD_DIM ** (-0.5)
                top = jnp.max(scores, axis=1, keepdims=True)
                wts = jnp.exp(scores - top)
                den = jnp.sum(wts, axis=1, keepdims=True)
                got = jnp.dot(wts.astype(BF16), vals, preferred_element_type=F32)
                out = jnp.where(mine, got / den, out)
            dst[:, at] = out.astype(BF16)
            return carry

        lax.fori_loop(first, last, group, 0)

    attend(q_ref, ctx, 0, groups)
    back = []
    for s in range(1, W):
        for g in range(groups):
            q_copies[(s - 1) * groups + g].wait_recv()
            attend(qin.at[s - 1], cret.at[s - 1], g, g + 1)
            back.append(
                remote(
                    cret.at[s - 1, :, lanes_of(g)],
                    cback.at[s - 1, :, lanes_of(g)],
                    bs.at[s - 1, g],
                    br.at[s - 1, g],
                    wide_dev(W - s),
                )
            )
    ap_load.wait()
    lang = lang_ref[:, pl.ds(pl.multiple_of(w_at * rows, LANES), rows)]
    tag = jnp.zeros_like(lang)
    for g in range(W):
        tag = jnp.where(lang == g, owner_ref[g], tag)
    tag = to_column(tag)
    for s in range(1, W):
        for g in range(groups):
            back[(s - 1) * groups + g].wait_recv()
        other = rem(w_at + s, W)
        ctx[...] = jnp.where(
            tag == other, cback[s - 1].astype(F32), ctx[...].astype(F32)
        ).astype(BF16)
    sent += q_copies + back

    def scatter_sum(k, produce, consume):
        copies = []
        core_cp = []
        hi_cp = []
        for c in range(C + 1):
            if c < C:
                produce(c)
                core_cp.append(
                    remote(
                        part.at[c, 1 - lo], core_in.at[k, c], core_s.at[k, c], core_r.at[k, c], core_dev
                    )
                )
            if c > 0:
                b = c - 1
                core_cp[b].wait_recv()
                part[b, lo] = (part[b, lo].astype(F32) + core_in[k, b].astype(F32)).astype(BF16)
                if b == 0:
                    hi_cp.append([])
                    early = [
                        remote(
                            part.at[0, lo, :, rem(d_at + s, D)],
                            early_in.at[k, s - 1],
                            ed_s.at[k, s - 1],
                            ed_r.at[k, s - 1],
                            dep_dev(s),
                        )
                        for s in range(1, D)
                    ]
                    continue
                hi_cp.append(
                    [
                        remote(
                            part.at[b, lo, rem(hi + s, H)],
                            hi_in.at[k, b, s - 1],
                            hi_s.at[k, b, s - 1],
                            hi_r.at[k, b, s - 1],
                            hi_dev(s),
                        )
                        for s in range(1, H)
                    ]
                )
        dep_cp = [[]]
        for c in range(1, C):
            held = part[c, lo, hi].astype(F32)
            for s in range(1, H):
                hi_cp[c][s - 1].wait_recv()
                held = held + hi_in[k, c, s - 1].astype(F32)
            part[c, lo, hi] = held.astype(BF16)
            dep_cp.append(
                [
                    remote(
                        part.at[c, lo, hi, rem(d_at + s, D)],
                        dep_in.at[k, c, s - 1],
                        dep_s.at[k, c, s - 1],
                        dep_r.at[k, c, s - 1],
                        dep_dev(s),
                    )
                    for s in range(1, D)
                ]
            )
            if c == C - 2:
                held = part[0, lo, :, d_at].astype(F32)
                for s in range(1, D):
                    early[s - 1].wait_recv()
                    held = held + early_in[k, s - 1].astype(F32)
                part[0, lo, :, d_at] = held.astype(BF16)
                hi_cp[0] = [
                    remote(
                        part.at[0, lo, rem(hi + s, H), d_at],
                        late_in.at[k, s - 1],
                        eh_s.at[k, s - 1],
                        eh_r.at[k, s - 1],
                        hi_dev(s),
                    )
                    for s in range(1, H)
                ]
        for c in [1, 0] + list(range(2, C)):
            held = part[c, lo, hi, d_at].astype(F32)
            if c == 0:
                for s in range(1, H):
                    hi_cp[0][s - 1].wait_recv()
                    held = held + late_in[k, s - 1].astype(F32)
            else:
                for s in range(1, D):
                    dep_cp[c][s - 1].wait_recv()
                    held = held + dep_in[k, c, s - 1].astype(F32)
            consume(c, held)
        copies += early
        for c in range(C):
            copies += [core_cp[c]] + hi_cp[c] + dep_cp[c]
        return copies

    def store_part(c, q, tile):
        for n in range(2 * H):
            part[c, n % 2, n // 2, q] = tile[n * tok : (n + 1) * tok].astype(BF16)

    def project(c):
        def one(q, carry):
            at = pl.ds(pl.multiple_of(q * quarter + c * cw, LANES), cw)
            store_part(c, q, jnp.dot(ctx[...], ap[:, at], preferred_element_type=F32))
            return carry

        lax.fori_loop(0, D, one, 0)

    dep_ag = {}
    hi_ag = {}
    core_ag = {}

    def forward_hi(j, c):
        q = rem(d_at + D - j, D)
        for s in range(1, H):
            hi_ag[s, j, c] = remote(
                xg.at[lo, hi, q, c],
                xg.at[lo, hi, q, c],
                agh_s.at[s - 1, j, c],
                agh_r.at[s - 1, j, c],
                hi_dev(s),
            )

    def forward_core(i, j, c):
        q = rem(d_at + D - j, D)
        h = rem(hi + H - i, H)
        core_ag[i, j, c] = remote(
            xg.at[lo, h, q, c],
            xg.at[lo, h, q, c],
            agc_s.at[i, j, c],
            agc_r.at[i, j, c],
            core_dev,
        )

    def add_residual(c, total):
        res = hid_ref[:, c * cw : (c + 1) * cw].astype(F32) + total
        xg[lo, hi, d_at, c] = res.astype(BF16)
        for s in range(1, D):
            dep_ag[s, c] = remote(
                xg.at[lo, hi, d_at, c],
                xg.at[lo, hi, d_at, c],
                agd_s.at[s - 1, c],
                agd_r.at[s - 1, c],
                dep_dev(s),
            )
        forward_hi(0, c)
        forward_core(0, 0, c)

    first = scatter_sum(0, project, add_residual)

    for j in range(1, D):
        for c in range(C):
            dep_ag[j, c].wait_recv()
            forward_hi(j, c)
            forward_core(0, j, c)
    for j in range(D):
        for c in range(C):
            for s in range(1, H):
                hi_ag[s, j, c].wait_recv()
                forward_core(s, j, c)
    for key in core_ag:
        core_ag[key].wait_recv()

    def norm_block(n, carry):
        l = n % 2
        h = n // 2
        acc = jnp.zeros((tok, cw), F32)
        for q in range(D):
            for c in range(C):
                x = xg[l, h, q, c].astype(F32)
                acc = acc + x * x
        inv = lax.rsqrt(jnp.sum(acc, axis=1, keepdims=True) * (1.0 / width) + norm_eps)
        at_rows = pl.ds(pl.multiple_of(n * tok, tok), tok)
        for q in range(D):
            for c in range(C):
                at = q * quarter + c * cw
                x = xg[l, h, q, c].astype(F32)
                nm[at_rows, at : at + cw] = (x * inv * gain_ref[:, at : at + cw]).astype(BF16)
        return carry

    lax.fori_loop(0, 2 * H, norm_block, 0)

    pieces = lax.dot_general(
        nm[...], rout[...].astype(BF16), (((1,), (1,)), ((), ())), preferred_element_type=F32
    )
    column = lax.broadcasted_iota(jnp.int32, pieces.shape, 1)
    named = rem(column, experts)
    id0 = to_column(ids_ref[0:1, :])
    id1 = to_column(ids_ref[1:2, :])
    logit0 = jnp.sum(jnp.where(named == id0, pieces, 0.0), axis=1, keepdims=True)
    logit1 = jnp.sum(jnp.where(named == id1, pieces, 0.0), axis=1, keepdims=True)
    gate0 = 1.0 / (1.0 + jnp.exp(logit1 - logit0))
    gate1 = 1.0 / (1.0 + jnp.exp(logit0 - logit1))
    gate = jnp.where(id0 == n_at, gate0, 0.0) + jnp.where(id1 == n_at, gate1, 0.0)

    win_load.wait()
    hidden = win.shape[1]
    step = 256 if hidden % 256 == 0 else LANES

    def enter(i, carry):
        at = pl.ds(pl.multiple_of(i * step, LANES), step)
        v = jnp.dot(nm[...], win[:, at], preferred_element_type=F32)
        act = 0.5 * v * (1.0 + jnp.tanh((2.0 / jnp.pi) ** 0.5 * (v + 0.044715 * v * v * v)))
        hact[:, at] = act.astype(BF16)
        return carry

    lax.fori_loop(0, hidden // step, enter, 0)

    for cp in first:
        cp.wait_send()
    wout_load.wait()

    def leave(c):
        def one(q, carry):
            at = pl.ds(pl.multiple_of(q * quarter + c * cw, LANES), cw)
            tile = jnp.dot(hact[...], wout[:, at], preferred_element_type=F32)
            store_part(c, q, tile * gate)
            return carry

        lax.fori_loop(0, D, one, 0)

    def finish(c, total):
        out_ref[:, c * cw : (c + 1) * cw] = (xg[lo, hi, d_at, c].astype(F32) + total).astype(BF16)

    second = scatter_sum(1, leave, finish)

    sent += second
    sent += list(dep_ag.values()) + list(hi_ag.values()) + list(core_ag.values())
    for cp in sent:
        cp.wait_send()


def shards(
    hidden_in,
    queries,
    lang_ids,
    owner_slot,
    enc_kv,
    attn_proj,
    norm_gain,
    router_proj,
    expert_ids,
    proj_in,
    proj_out,
):
    W = lax.axis_size("wide")
    N = lax.axis_size("narrow")
    D = lax.axis_size("depth")
    H = N // 2
    C = CHUNKS
    rows, feats = queries.shape
    tok, quarter = hidden_in.shape
    cw = quarter // C
    width = quarter * D
    assert owner_slot.shape[0] == W and enc_kv.shape[0] == 1 and proj_in.shape[0] == 1 and N % 2 == 0
    experts = router_proj.shape[1]
    hidden = proj_in.shape[2]
    keys = enc_kv.shape[2]
    dma = pltpu.SemaphoreType.DMA
    vmem = pl.BlockSpec(memory_space=pltpu.VMEM)
    hbm = pl.BlockSpec(memory_space=pl.ANY)
    smem = pl.BlockSpec(memory_space=pltpu.SMEM)
    return pl.pallas_call(
        functools.partial(layer_kernel, (W, H, D)),
        out_shape=jax.ShapeDtypeStruct((tok, quarter), BF16),
        in_specs=[smem] + [vmem] * 6 + [hbm] * 4,
        out_specs=vmem,
        scratch_shapes=[
            pltpu.VMEM((2, keys, feats), BF16),
            pltpu.VMEM(attn_proj.shape, BF16),
            pltpu.VMEM(proj_in.shape[1:], BF16),
            pltpu.VMEM(proj_out.shape[1:], BF16),
            pltpu.VMEM((W - 1, rows, feats), BF16),
            pltpu.VMEM((W - 1, rows, feats), BF16),
            pltpu.VMEM((W - 1, rows, feats), BF16),
            pltpu.VMEM((rows, feats), BF16),
            pltpu.VMEM((C, 2, H, D, tok, cw), BF16),
            pltpu.VMEM((2, C, H, D, tok, cw), BF16),
            pltpu.VMEM((2, C, H - 1, D, tok, cw), BF16),
            pltpu.VMEM((2, C, D - 1, tok, cw), BF16),
            pltpu.VMEM((2, H, D, C, tok, cw), BF16),
            pltpu.VMEM((rows, width), BF16),
            pltpu.VMEM((rows, hidden), BF16),
            pltpu.VMEM((-(-3 * experts // 16) * 16, width), F32),
            pltpu.VMEM((2, D - 1, H, tok, cw), BF16),
            pltpu.VMEM((2, H - 1, tok, cw), BF16),
            dma((2, D - 1)),
            dma((2, D - 1)),
            dma((2, H - 1)),
            dma((2, H - 1)),
            dma((4,)),
            dma((W - 1, feats // LANES)),
            dma((W - 1, feats // LANES)),
            dma((W - 1, feats // LANES)),
            dma((W - 1, feats // LANES)),
            dma((2, C)),
            dma((2, C)),
            dma((2, C, H - 1)),
            dma((2, C, H - 1)),
            dma((2, C, D - 1)),
            dma((2, C, D - 1)),
            dma((D - 1, C)),
            dma((D - 1, C)),
            dma((H - 1, D, C)),
            dma((H - 1, D, C)),
            dma((H, D, C)),
            dma((H, D, C)),
        ],
        compiler_params=pltpu.CompilerParams(
            collective_id=0, has_side_effects=True, vmem_limit_bytes=67043328
        ),
    )(
        owner_slot,
        lang_ids.reshape(1, -1),
        queries,
        hidden_in,
        norm_gain.reshape(1, width),
        router_proj.T,
        expert_ids.T,
        enc_kv,
        attn_proj,
        proj_in,
        proj_out,
    )


def solution(mesh):
    return jax.shard_map(
        shards,
        mesh=mesh,
        in_specs=(
            P(("wide", "narrow"), "depth"),
            P("wide", ("narrow", "depth")),
            P(),
            P(),
            P("wide", None, None, ("narrow", "depth")),
            P(("narrow", "depth"), None),
            P(),
            P(),
            P("wide", None),
            P("narrow", None, "depth"),
            P("narrow", "depth", None),
        ),
        out_specs=P(("wide", "narrow"), "depth"),
        check_vma=False,
    )
```
